32 devices in a mesh: expert: 8 (over y, x, core), shard: 4 (over z).
Axes of the slice: x: 2, y: 2, z: 4, core: 2. Of those that a mesh axis runs over, the one named last changes fastest.
Arguments:
- w_gate: float32 [64, 2048, 1024], P('expert', 'shard'), may hold values from -0.1875 to 0.1875
- avg_gate: float32 [64, 2048, 1024], P('expert', 'shard'), may hold values from -0.125 to 0.125
- w_up: float32 [64, 2048, 1024], P('expert', 'shard'), may hold values from -0.1875 to 0.1875
- avg_up: float32 [64, 2048, 1024], P('expert', 'shard'), may hold values from -0.125 to 0.125
- mix_share: float32 [64], P('expert'), may hold values from 0.2 to 0.8
- router_weight: float32 [2048, 64], P('shard', 'expert'), may hold values from -0.125 to 0.125
- router_gain: float32 [2048], P('shard'), may hold values from 0.25 to 1.75
Outputs:
- serve_gate: bfloat16 [64, 2048, 1024], P('expert')
- serve_up: bfloat16 [64, 2048, 1024], P('expert')
- scale_gate: float32 [64, 1024], P('expert')
- scale_up: float32 [64, 1024], P('expert')
- serve_router: bfloat16 [2048, 64], replicated
The draws below stay inside these ranges and needn't reach their ends.
All inputs are finite; a program needn't handle non-finite values.
Results may differ from the reference program's by a relative error of at most 0.001.
Values may be sent and summed in bfloat16 or wider, within the bound.
A program may use at most 256 MiB of HBM per device.

```python
import jax
import jax.numpy as jnp
from jax import lax

EXPERTS = 64
D_MODEL = 2048
D_EXPERT = 1024


def with_spikes(result, own_key, source, target, parts, factor):
    def block_of(position):
        return (jnp.arange(result.shape[position]) // (result.shape[position] // parts)).reshape((-1,) + (1,) * (result.ndim - 1 - position))

    first = jax.random.permutation(own_key, parts)[block_of(target)]
    second = (block_of(target) + parts // 2) % parts
    return jnp.where((block_of(source) == first) | (block_of(source) == second), factor * result, result)


def level_of(stream_key, dims, shards, low, top_value):
    def one(dim, parts):
        steps = jax.random.uniform(jax.random.fold_in(jax.random.fold_in(stream_key, 6), dim), (parts,), jnp.float32, low / len(shards), top_value / len(shards))
        return jnp.repeat(jnp.exp(steps), dims[dim] // parts).reshape((-1,) + (1,) * (len(dims) - dim - 1))

    gain = one(*shards[0])
    for cut in shards[1:]:
        gain = gain * one(*cut)
    return gain


def normal_values(own_key, extent, width, reach, pieces=(), kind=jnp.bfloat16):
    level = level_of(own_key, extent, pieces, -0.22, 0.18) if pieces else 1.0
    values = jax.random.normal(own_key, extent, jnp.float32) * width * level
    return jnp.minimum(jnp.maximum(values, -reach), reach).astype(kind)


def noise_with(stream_key, extent, scale, bound, shards, heavy, dtype=jnp.bfloat16):
    values = scale * jax.random.normal(stream_key, extent, jnp.float32)
    if shards:
        values = values * level_of(stream_key, extent, shards, -0.22, 0.18)
    return jnp.clip(with_spikes(values, jax.random.fold_in(stream_key, 3), *heavy), -bound, bound).astype(dtype)


def setup_inputs(seed: int = 0) -> dict:
    key_of = jax.random.split(jax.random.key(seed), 8)
    return {
        "w_gate": noise_with(key_of[0], (EXPERTS, D_MODEL, D_EXPERT), D_MODEL ** -0.5, 0.1875, ((0, 8), (1, 4)), (1, 2, 4, 2.0), jnp.float32),
        "avg_gate": normal_values(key_of[1], (EXPERTS, D_MODEL, D_EXPERT), D_MODEL ** -0.5, 0.125, ((0, 8), (1, 4)), jnp.float32),
        "w_up": noise_with(key_of[2], (EXPERTS, D_MODEL, D_EXPERT), D_MODEL ** -0.5, 0.1875, ((0, 8), (1, 4)), (1, 2, 4, 2.0), jnp.float32),
        "avg_up": normal_values(key_of[3], (EXPERTS, D_MODEL, D_EXPERT), D_MODEL ** -0.5, 0.125, ((0, 8), (1, 4)), jnp.float32),
        "mix_share": jnp.clip(0.2 + 0.6 * jax.random.uniform(key_of[4], (EXPERTS,), jnp.float32) ** level_of(key_of[4], (EXPERTS,), ((0, 8),), -0.2, 0.2), 0.2, 0.8),
        "router_weight": normal_values(key_of[5], (D_MODEL, EXPERTS), D_MODEL ** -0.5, 0.125, ((0, 4), (1, 8)), jnp.float32),
        "router_gain": jnp.clip(1.0 + 0.15 * jax.random.normal(key_of[6], (D_MODEL,), jnp.float32), 0.25, 1.75),
    }


def reference(w_gate, avg_gate, w_up, avg_up, mix_share, router_weight, router_gain):
    fresh_gate = mix_share[:, None, None] * w_gate + (1.0 - mix_share[:, None, None]) * avg_gate
    fresh_up = mix_share[:, None, None] * w_up + (1.0 - mix_share[:, None, None]) * avg_up
    scale_gate = jnp.sqrt(lax.optimization_barrier(jnp.sum(fresh_gate * fresh_gate, axis=1)))
    serve_gate = (fresh_gate / jnp.expand_dims(scale_gate, 1)).astype(jnp.bfloat16)
    scale_up = jnp.sqrt(lax.optimization_barrier(jnp.sum(fresh_up * fresh_up, axis=1)))
    serve_up = (fresh_up / jnp.expand_dims(scale_up, 1)).astype(jnp.bfloat16)
    serve_router = (router_weight * router_gain[:, None]).astype(jnp.bfloat16)
    return (serve_gate, serve_up, scale_gate, scale_up, serve_router)
```

```python
import functools

import jax
import jax.numpy as jnp
from jax import lax
from jax.experimental import pallas as pl
from jax.experimental.pallas import tpu as pltpu
from jax.sharding import PartitionSpec as P

MESH = pl.DeviceIdType.MESH
SLOTS = 4
ROWS = 16


def kernel(
    ns, experts, rows, mix_ref, wg_ref, ag_ref, wu_ref, au_ref,
    og_ref, ou_ref, sg_ref, su_ref,
    fresh, other, narrow, head, tail,
    w_sem, a_sem, local_sem, recv_sem, right_sem, left_sem, head_send, head_recv, tail_send, tail_recv,
):
    z = lax.axis_index("shard")
    n = 2 * experts
    firsts, seconds, outs, scales = (wg_ref, wu_ref), (ag_ref, au_ref), (og_ref, ou_ref), (sg_ref, su_ref)

    barrier = pltpu.get_barrier_semaphore()
    for k in range(1, ns):
        pl.semaphore_signal(barrier, inc=1, device_id={"shard": lax.rem(z + k, ns)}, device_id_type=MESH)

    def w_copy(e, which):
        c = 2 * e + which
        return pltpu.make_async_copy(firsts[which].at[e], fresh.at[c], w_sem.at[c])

    def a_copy(e, which):
        slot = lax.rem(2 * e + which, SLOTS)
        return pltpu.make_async_copy(seconds[which].at[e], other.at[slot], a_sem.at[slot])

    def place(e, which, j):
        return outs[which].at[e, pl.ds(pl.multiple_of(j * rows, rows), rows), :]

    def local_copy(e, which):
        c = 2 * e + which
        return pltpu.make_async_copy(narrow.at[c], place(e, which, z), local_sem.at[c])

    def to_right(e, which, d):
        c = 2 * e + which
        src = narrow.at[c] if d == 0 else place(e, which, z - d)
        return pltpu.make_async_remote_copy(
            src_ref=src, dst_ref=place(e, which, z - d), send_sem=right_sem.at[d, c],
            recv_sem=recv_sem.at[z - d, c], device_id={"shard": z + 1}, device_id_type=MESH,
        )

    def to_left(e, which, d):
        c = 2 * e + which
        src = narrow.at[c] if d == 0 else place(e, which, z + d)
        return pltpu.make_async_remote_copy(
            src_ref=src, dst_ref=place(e, which, z + d), send_sem=left_sem.at[d, c],
            recv_sem=recv_sem.at[z + d, c], device_id={"shard": z - 1}, device_id_type=MESH,
        )

    def arrival(e, which, j):
        c = 2 * e + which
        return pltpu.make_async_copy(place(e, which, j), place(e, which, j), recv_sem.at[j, c])

    def sums_to(part, send, recv, k):
        return pltpu.make_async_remote_copy(
            src_ref=part.at[z], dst_ref=part.at[z], send_sem=send.at[k], recv_sem=recv.at[z],
            device_id={"shard": lax.rem(z + k, ns)}, device_id_type=MESH,
        )

    def sums_from(part, recv, k):
        j = lax.rem(z + k, ns)
        return pltpu.make_async_copy(part.at[j], part.at[j], recv.at[j])

    def mix(e, which, part, row):
        c = 2 * e + which
        slot = lax.rem(c, SLOTS)
        w_copy(e, which).wait()
        a_copy(e, which).wait()
        share = mix_ref[e]
        rest = 1.0 - share

        def step(i, acc):
            r = pl.ds(pl.multiple_of(i * ROWS, ROWS), ROWS)
            value = share * fresh[c, r, :] + rest * other[slot, r, :]
            fresh[c, r, :] = value
            square = value * value
            for k in range(0, ROWS, 8):
                acc = acc + square[k : k + 8]
            return acc

        acc = lax.fori_loop(0, rows // ROWS, step, jnp.zeros((8, fresh.shape[2]), jnp.float32), unroll=2)
        part[z, pl.ds(row, 1), :] = jnp.sum(acc, axis=0, keepdims=True)

    def finish(e, which, part, row):
        c = 2 * e + which
        total = part[0, pl.ds(row, 1), :]
        for j in range(1, ns):
            total = total + part[j, pl.ds(row, 1), :]
        scale = jnp.sqrt(total)
        scales[which][pl.ds(e, 1), :] = scale
        wide = jnp.broadcast_to(scale, (8, scale.shape[1]))
        wide = jnp.concatenate([wide] * (ROWS // 8), axis=0)

        def step(i, carry):
            r = pl.ds(pl.multiple_of(i * ROWS, ROWS), ROWS)
            narrow[c, r, :] = (fresh[c, r, :] / wide).astype(jnp.bfloat16)
            return carry

        lax.fori_loop(0, rows // ROWS, step, 0, unroll=2)

        @pl.when(z < ns - 1)
        def _():
            to_right(e, which, 0).start()

        @pl.when(z > 0)
        def _():
            to_left(e, which, 0).start()

        local_copy(e, which).start()

    for c in range(min(SLOTS, n)):
        w_copy(c // 2, c % 2).start()
        a_copy(c // 2, c % 2).start()
    for c in range(SLOTS, n):
        w_copy(c // 2, c % 2).start()

    def refill(e, which):
        if experts > SLOTS // 2:
            @pl.when(e + SLOTS // 2 < experts)
            def _():
                a_copy(e + SLOTS // 2, which).start()

    mix(0, 0, head, 0)
    refill(0, 0)
    mix(0, 1, head, 1)
    refill(0, 1)
    pl.semaphore_wait(barrier, ns - 1)
    for k in range(1, ns):
        sums_to(head, head_send, head_recv, k).start()
    if experts > 1:
        mix(1, 0, tail, 0)
        refill(1, 0)
    for k in range(1, ns):
        sums_from(head, head_recv, k).wait()
    finish(0, 0, head, 0)
    if experts > 1:
        mix(1, 1, tail, 1)
        refill(1, 1)

        def more(e, carry):
            for which in range(2):
                mix(e, which, tail, 2 * (e - 1) + which)
                refill(e, which)
            return carry

        lax.fori_loop(2, experts, more, 0)
        for k in range(1, ns):
            sums_to(tail, tail_send, tail_recv, k).start()
    finish(0, 1, head, 1)
    if experts > 1:
        for k in range(1, ns):
            sums_from(tail, tail_recv, k).wait()

        def rest(e, carry):
            for which in range(2):
                finish(e, which, tail, 2 * (e - 1) + which)
            return carry

        lax.fori_loop(1, experts, rest, 0)

    for d in range(1, ns):
        def pass_on(e, carry, d=d):
            for which in range(2):
                @pl.when(z >= d)
                def _():
                    arrival(e, which, z - d).wait()

                @pl.when(z + d < ns)
                def _():
                    arrival(e, which, z + d).wait()

                if d < ns - 1:
                    @pl.when((z >= d) & (z < ns - 1))
                    def _():
                        to_right(e, which, d).start()

                    @pl.when((z + d < ns) & (z > 0))
                    def _():
                        to_left(e, which, d).start()
            return carry

        lax.fori_loop(0, experts, pass_on, 0)

    def drain(e, carry):
        for which in range(2):
            local_copy(e, which).wait()
            for d in range(ns - 1):
                @pl.when((z >= d) & (z < ns - 1))
                def _():
                    to_right(e, which, d).wait_send()

                @pl.when((z + d < ns) & (z > 0))
                def _():
                    to_left(e, which, d).wait_send()
        return carry

    lax.fori_loop(0, experts, drain, 0)
    for k in range(1, ns):
        sums_to(head, head_send, head_recv, k).wait_send()
        if experts > 1:
            sums_to(tail, tail_send, tail_recv, k).wait_send()


def solution(mesh):
    ns, ne = mesh.shape["shard"], mesh.shape["expert"]

    def per_device(w_gate, avg_gate, w_up, avg_up, mix_share, router_weight, router_gain):
        experts, rows, cols = w_gate.shape
        n = 2 * experts
        dma = pltpu.SemaphoreType.DMA
        anywhere = pl.BlockSpec(memory_space=pl.ANY)
        vmem = pl.BlockSpec(memory_space=pltpu.VMEM)
        serve = jax.ShapeDtypeStruct((experts, ns * rows, cols), jnp.bfloat16)
        scale = jax.ShapeDtypeStruct((experts, cols), jnp.float32)

        part_router = (router_weight * router_gain[:, None]).astype(jnp.bfloat16).T
        every = lax.all_gather(part_router, ("shard", "expert"), axis=0, tiled=False)
        every = every.reshape(ns, ne, part_router.shape[0], rows)
        serve_router = every.transpose(0, 3, 1, 2).reshape(ns * rows, ne * part_router.shape[0])

        serve_gate, serve_up, scale_gate, scale_up = pl.pallas_call(
            functools.partial(kernel, ns, experts, rows),
            out_shape=(serve, serve, scale, scale),
            in_specs=[pl.BlockSpec(memory_space=pltpu.SMEM)] + [anywhere] * 4,
            out_specs=(anywhere, anywhere, vmem, vmem),
            scratch_shapes=[
                pltpu.VMEM((n, rows, cols), jnp.float32),
                pltpu.VMEM((SLOTS, rows, cols), jnp.float32),
                pltpu.VMEM((n, rows, cols), jnp.bfloat16),
                pltpu.VMEM((ns, 2, cols), jnp.float32),
                pltpu.VMEM((ns, max(n - 2, 1), cols), jnp.float32),
                dma((n,)),
                dma((SLOTS,)),
                dma((n,)),
                dma((ns, n)),
                dma((ns - 1, n)),
                dma((ns - 1, n)),
                dma((ns,)),
                dma((ns,)),
                dma((ns,)),
                dma((ns,)),
            ],
            compiler_params=pltpu.CompilerParams(
                collective_id=0, has_side_effects=True, vmem_limit_bytes=62 * 1024 * 1024
            ),
        )(mix_share, w_gate, avg_gate, w_up, avg_up)
        return serve_gate, serve_up, scale_gate, scale_up, serve_router

    return jax.shard_map(
        per_device,
        mesh=mesh,
        in_specs=(
            P("expert", "shard", None),
            P("expert", "shard", None),
            P("expert", "shard", None),
            P("expert", "shard", None),
            P("expert"),
            P("shard", "expert"),
            P("shard"),
        ),
        out_specs=(
            P("expert", None, None),
            P("expert", None, None),
            P("expert", None),
            P("expert", None),
            P(),
        ),
        check_vma=False,
    )
```
